1024 devices in a mesh: blk: 64 (over z, x), hub: 8 (over y), rep: 2 (over core).
Axes of the slice: x: 4, y: 8, z: 16, core: 2. Of those that a mesh axis runs over, the one named last changes fastest.
Arguments:
- source_feats: bfloat16 [262144, 512], P(('blk', 'hub', 'rep')), may hold values from -6 to 6
- target_feats: bfloat16 [524288, 512], P(('blk', 'hub', 'rep')), may hold values from -6 to 6
- hub_feats: bfloat16 [16384, 512], P(('blk', 'hub', 'rep')), may hold values from -6 to 6
- weight_self: bfloat16 [512, 256], replicated, may hold values from -0.25 to 0.25
- weight_neigh: bfloat16 [512, 256], replicated, may hold values from -0.25 to 0.25
- bias_vector: float32 [256], replicated, may hold values from -3 to 3
- send_rows: int32 [1024, 64, 32], P(('blk', 'hub', 'rep')), may hold values from 0 to 255
- edge_target: int32 [1024, 4096], P(('blk', 'hub', 'rep')), may hold values from 0 to 511
- edge_slot: int32 [1024, 4096], P(('blk', 'hub', 'rep')), may hold values from 0 to 2303, as said below
- hub_source: int32 [1024, 512], P(('blk', 'hub', 'rep')), may hold values from 0 to 255
- hub_target: int32 [1024, 512], P(('blk', 'hub', 'rep')), may hold values from 0 to 255
Outputs:
- vertex_out: bfloat16 [524288, 256], P(('blk', 'hub', 'rep'))
- hub_out: bfloat16 [16384, 256], P(('blk', 'hub', 'rep'))
The draws below stay inside these ranges and needn't reach their ends.
Inputs may be any that keep to these rules, and one draw needn't show every extreme that they name: `edge_slot`: A value s < 2048 names slot s of table_d (row s % 32 of the block that blk index s // 32 sends); larger values name hubs of the device's blk index. For each device and blk index the slots named lie within a prefix of that block, of uneven length.
All inputs are finite; a program needn't handle non-finite values.
Results may differ from the reference program's by a relative error of at most 0.0025.
Values may be sent and summed in bfloat16 or wider, within the bound.
A program may use at most 32 MiB of HBM per device.

```python
import math
import jax
import jax.numpy as jnp
import numpy as np
from jax import lax

FEAT = 512
HIDDEN_SIZE = 256
CAP = 32
SRC_DEV = 256
DST_DEV = 512
E_DEV = 4096
EH_DEV = 512
G_HUB = 256
NSRC = 262144
NDST = 524288
NHUB = 16384
N_BLK = 64
N_HUB = 8
N_REP = 2
DEVICES = 1024


def draw_edge_slot(key, part):
    keys = jax.random.split(key, 6)
    lengths = jax.random.randint(keys[0], (DEVICES, N_BLK), 1, CAP + 1)
    longest = jax.random.randint(keys[1], (DEVICES, 1), 0, N_BLK)
    lengths = jnp.where(jnp.arange(N_BLK)[None, :] == longest, CAP, lengths)
    peer = jax.random.randint(keys[2], (DEVICES, E_DEV), 0, N_BLK)
    raw = jax.random.randint(keys[3], (DEVICES, E_DEV), 0, 1 << 20)
    within = raw % jnp.take_along_axis(lengths, peer, axis=1)
    hubpick = jax.random.randint(keys[4], (DEVICES, E_DEV), 0, G_HUB)
    chooser = jax.random.randint(keys[5], (DEVICES, E_DEV), 0, 8)
    return jnp.where(chooser == 0, N_BLK * CAP + hubpick, peer * CAP + within).astype(jnp.int32)


def with_ends(entries, key, smallest, largest):
    longest = entries.shape.index(max(entries.shape))
    spots = []
    for shift in (0, 1):
        where = [jax.random.randint(jax.random.fold_in(key, axis), (), 0, length) for axis, length in enumerate(entries.shape)]
        where[longest] = (where[longest] + shift) % entries.shape[longest]
        spots.append(tuple(where))
    return entries.at[spots[0]].set(smallest).at[spots[1]].set(largest)


def block_scale(rng, extent, cuts, least, top_value):
    loudness, own = 1.0, jax.random.fold_in(rng, 6)
    for axis_at, blocks in cuts:
        draws = jnp.exp(jax.random.uniform(jax.random.fold_in(own, axis_at), (blocks,), jnp.float32, least / len(cuts), top_value / len(cuts)))
        loudness = loudness * jnp.repeat(draws, extent[axis_at] // blocks).reshape([-1 if axis == axis_at else 1 for axis in range(len(extent))])
    return loudness


def cumulative_ranks(amount, lean):
    portions = [(1 << 20) // math.isqrt(standing ** lean) + 1 for standing in range(1, amount + 1)]
    width = 1 + sum(portions) // (1 << 30)
    return np.cumsum(np.array([max(1, weight // width) for weight in portions]))


def ranked_ids(stream_key, dims, number_of, lean):
    grid = cumulative_ranks(number_of, lean)
    pick = jax.random.randint(jax.random.fold_in(stream_key, 1), dims, 0, int(grid[number_of - 1]))
    grade = jnp.searchsorted(jnp.asarray(grid, jnp.int32), pick, side="right")
    return jax.random.permutation(jax.random.fold_in(stream_key, 2), number_of)[grade].astype(jnp.int32)


def scatter_about(rng, extent, scale, bound, pieces=(), held_as=jnp.bfloat16):
    array = jax.random.normal(rng, extent, jnp.float32) * scale
    if len(pieces) > 0:
        array = block_scale(rng, extent, pieces, -0.22, 0.18) * array
    return jnp.clip(array, min=-bound, max=bound).astype(held_as)


def setup_inputs(seed: int = 0) -> dict:
    splits = jax.random.split(jax.random.key(seed), 12)
    source_feats = scatter_about(splits[0], (NSRC, FEAT), 1.0, 6.0, ((0, 1024),))
    target_feats = scatter_about(splits[1], (NDST, FEAT), 1.0, 6.0, ((0, 1024),))
    hub_feats = scatter_about(splits[2], (NHUB, FEAT), 1.0, 6.0, ((0, 1024),))
    weight_self = scatter_about(splits[3], (FEAT, HIDDEN_SIZE), FEAT ** -0.5, 0.25)
    weight_neigh = scatter_about(splits[4], (FEAT, HIDDEN_SIZE), FEAT ** -0.5, 0.25)
    bias_vector = scatter_about(splits[5], (HIDDEN_SIZE,), 0.5, 3.0, (), jnp.float32)
    send_rows = with_ends(jax.random.randint(splits[6], (DEVICES, N_BLK, CAP), 0, SRC_DEV), jax.random.fold_in(splits[6], 1), 0, SRC_DEV - 1).astype(jnp.int32)
    edge_target = with_ends(jax.random.randint(splits[7], (DEVICES, E_DEV), 0, DST_DEV), jax.random.fold_in(splits[7], 1), 0, DST_DEV - 1).astype(jnp.int32)
    edge_slot = draw_edge_slot(jax.random.fold_in(splits[11], 71), 0)
    hub_source = with_ends(jax.random.randint(splits[9], (DEVICES, EH_DEV), 0, SRC_DEV), jax.random.fold_in(splits[9], 1), 0, SRC_DEV - 1).astype(jnp.int32)
    hub_target = with_ends(ranked_ids(splits[10], (DEVICES, EH_DEV), G_HUB, 2), jax.random.fold_in(splits[10], 3), 0, G_HUB - 1).astype(jnp.int32)
    return dict(source_feats=source_feats, target_feats=target_feats, hub_feats=hub_feats, weight_self=weight_self, weight_neigh=weight_neigh, bias_vector=bias_vector, send_rows=send_rows, edge_target=edge_target, edge_slot=edge_slot, hub_source=hub_source, hub_target=hub_target)


def reference(source_feats, target_feats, hub_feats, weight_self, weight_neigh, bias_vector, send_rows, edge_target, edge_slot, hub_source, hub_target):
    groups = N_HUB * N_REP
    total = N_BLK * groups
    source_proj = jnp.dot(source_feats, weight_neigh, preferred_element_type=jnp.float32).astype(jnp.bfloat16)
    hub_proj = jnp.dot(hub_feats, weight_neigh, preferred_element_type=jnp.float32).astype(jnp.bfloat16)
    proj_grid = source_proj.reshape(N_BLK, groups, SRC_DEV, HIDDEN_SIZE)
    send_grid = send_rows.reshape(N_BLK, groups, N_BLK, CAP)
    peers = jnp.arange(N_BLK, dtype=jnp.int32)

    def per_device(device):
        blk_index = device // groups
        member = device % groups
        picked = send_grid[:, member, blk_index, :]
        arrived = proj_grid[peers[:, None], member, picked]
        hubs = lax.dynamic_slice_in_dim(hub_proj, (blk_index * G_HUB).astype(jnp.int32), G_HUB, 0)
        table = jnp.concatenate([arrived.reshape(N_BLK * CAP, HIDDEN_SIZE), hubs], axis=0)
        gathered = table[edge_slot[device]].astype(jnp.float32)
        neigh_sum = jax.ops.segment_sum(gathered, edge_target[device], DST_DEV)
        degree = jax.ops.segment_sum(jnp.ones((E_DEV,), jnp.float32), edge_target[device], DST_DEV)
        rows = lax.dynamic_slice_in_dim(target_feats, (device * DST_DEV).astype(jnp.int32), DST_DEV, 0)
        own = jnp.dot(rows, weight_self, preferred_element_type=jnp.float32)
        result = own + neigh_sum / jnp.maximum(degree, 1.0)[:, None] + bias_vector[None, :]
        return jnp.maximum(result, 0.0).astype(jnp.bfloat16)

    vertex_out = lax.map(per_device, jnp.arange(total, dtype=jnp.int32)).reshape(total * DST_DEV, HIDDEN_SIZE)
    src_grid = hub_source.reshape(N_BLK, groups, EH_DEV)
    dst_grid = hub_target.reshape(N_BLK, groups, EH_DEV)
    members = jnp.arange(groups, dtype=jnp.int32)

    def per_block(blk_index):
        rows = proj_grid[blk_index][members[:, None], src_grid[blk_index]]
        flat = rows.reshape(groups * EH_DEV, HIDDEN_SIZE).astype(jnp.float32)
        keys = dst_grid[blk_index].reshape(groups * EH_DEV)
        hub_sum = jax.ops.segment_sum(flat, keys, G_HUB)
        hub_degree = jax.ops.segment_sum(jnp.ones((groups * EH_DEV,), jnp.float32), keys, G_HUB)
        return hub_sum, hub_degree

    hub_sum, hub_degree = lax.map(per_block, jnp.arange(N_BLK, dtype=jnp.int32))
    hub_sum = hub_sum.reshape(N_BLK * G_HUB, HIDDEN_SIZE)
    hub_degree = hub_degree.reshape(N_BLK * G_HUB)
    own_hub = jnp.dot(hub_feats, weight_self, preferred_element_type=jnp.float32)
    hub_out = jnp.maximum(own_hub + hub_sum / jnp.maximum(hub_degree, 1.0)[:, None] + bias_vector[None, :], 0.0).astype(jnp.bfloat16)
    return vertex_out, hub_out
```

```python
import jax
import jax.numpy as jnp
from jax import lax
from jax.sharding import PartitionSpec as P

NZ, NX = 16, 4


def one_hot(ids, count):
    return (ids[None, :] == jnp.arange(count, dtype=jnp.int32)[:, None]).astype(jnp.bfloat16)


def dot(a, b, dims):
    return lax.dot_general(a, b, dims, preferred_element_type=jnp.float32)


def on_device(
    source_feats,
    target_feats,
    hub_feats,
    weight_self,
    weight_neigh,
    bias_vector,
    send_rows,
    edge_target,
    edge_slot,
    hub_source,
    hub_target,
):
    width = weight_neigh.shape[1]
    rows = source_feats.shape[0]
    cap = send_rows.shape[2]
    targets = target_feats.shape[0]
    group = lax.axis_size(("hub", "rep"))
    mine = hub_feats.shape[0]
    hubs = group * mine
    nz, nx = NZ, NX
    z_groups = [[z * nx + x for z in range(nz)] for x in range(nx)]
    x_groups = [[z * nx + x for x in range(nx)] for z in range(nz)]
    z = lax.axis_index("blk") // nx

    proj = jnp.dot(source_feats, weight_neigh, preferred_element_type=jnp.float32).astype(jnp.bfloat16)
    picked = send_rows[0].reshape(-1, width).astype(jnp.bfloat16)
    payload = jnp.concatenate([proj, picked], axis=0)
    column = lax.all_gather(payload, "blk", axis=0, tiled=False, axis_index_groups=z_groups)

    hub_local = jnp.dot(hub_feats, weight_neigh, preferred_element_type=jnp.float32).astype(jnp.bfloat16)
    hub_rows = dot(one_hot(hub_source[0], rows), proj, (((0,), (0,)), ((), ()))).astype(jnp.bfloat16)
    hub_select = one_hot(hub_target[0], hubs)
    hub_partial = dot(hub_select, hub_rows, (((1,), (0,)), ((), ())))
    hub_edges = jnp.sum(hub_select.astype(jnp.float32), axis=1)
    parts = jnp.concatenate(
        [
            hub_partial.reshape(group, mine, width),
            jnp.broadcast_to(hub_local.astype(jnp.float32)[None], (group, mine, width)),
            jnp.pad(hub_edges.reshape(group, 1, mine), ((0, 0), (0, 7), (0, width - mine))),
        ],
        axis=1,
    )
    got = lax.all_to_all(parts, ("hub", "rep"), 0, 0, tiled=True)
    hub_sum = jnp.sum(got[:, :mine], axis=0)
    hub_table = got[:, mine : 2 * mine].reshape(hubs, width).astype(jnp.bfloat16)
    hub_degree = jnp.sum(got[:, 2 * mine, :mine], axis=0)

    slots = nz * nx * cap + hubs
    select_t = one_hot(edge_target[0], targets)
    counts = dot(select_t, one_hot(edge_slot[0], slots), (((1,), (1,)), ((), ())))
    high = jnp.floor(counts * (1.0 / 256.0))
    low = (counts - 256.0 * high).astype(jnp.bfloat16)
    high = high.astype(jnp.bfloat16)
    degree = jnp.sum(select_t.astype(jnp.float32), axis=1)
    own = jnp.dot(target_feats, weight_self, preferred_element_type=jnp.float32)

    ids = column[:, rows:, :].reshape(nz, nz, nx * cap)
    ids = lax.dynamic_index_in_dim(ids, z, 1, keepdims=False)
    pick = (
        ids[:, :, None] == jnp.arange(rows, dtype=jnp.int32)[None, None, :].astype(jnp.bfloat16)
    ).astype(jnp.bfloat16)
    blocks = dot(pick, column[:, :rows, :], (((2,), (1,)), ((0,), (0,)))).astype(jnp.bfloat16)
    outgoing = blocks.reshape(nz, nx, cap, width).transpose(1, 0, 2, 3)
    arrived = lax.all_to_all(outgoing, "blk", 0, 0, tiled=True, axis_index_groups=x_groups)
    arrived = arrived.transpose(1, 0, 2, 3).reshape(nz * nx * cap, width)
    table = jnp.concatenate([arrived, hub_table], axis=0)
    neigh_sum = jnp.dot(low, table, preferred_element_type=jnp.float32) + 256.0 * jnp.dot(
        high, table, preferred_element_type=jnp.float32
    )
    vertex_out = jnp.maximum(
        own + neigh_sum / jnp.maximum(degree, 1.0)[:, None] + bias_vector[None, :], 0.0
    ).astype(jnp.bfloat16)
    own_hub = jnp.dot(hub_feats, weight_self, preferred_element_type=jnp.float32)
    hub_out = jnp.maximum(
        own_hub + hub_sum / jnp.maximum(hub_degree, 1.0)[:, None] + bias_vector[None, :], 0.0
    ).astype(jnp.bfloat16)
    return (vertex_out, hub_out)


def solution(mesh):
    rows2 = P(("blk", "hub", "rep"), None)
    in_specs = (
        rows2, rows2, rows2, P(), P(), P(),
        P(("blk", "hub", "rep"), None, None),
        rows2, rows2, rows2, rows2,
    )
    return jax.shard_map(
        on_device, mesh=mesh, in_specs=in_specs, out_specs=(rows2, rows2), check_vma=False
    )
```

```python
import functools

import jax
import jax.numpy as jnp
from jax import lax
from jax.experimental import pallas as pl
from jax.experimental.pallas import tpu as pltpu
from jax.sharding import PartitionSpec as P

MESH = pl.DeviceIdType.MESH
NZ, NX = 16, 4
CHUNKS = 4
LANES = 128
BF, F32 = jnp.bfloat16, jnp.float32


def dot(a, b, contract):
    return lax.dot_general(a, b, ((contract[:1], contract[1:]), ((), ())), preferred_element_type=F32)


def one_hot(ids, first, count):
    rows = lax.broadcasted_iota(jnp.int32, (count, ids.shape[1]), 0)
    return jnp.where(rows == ids - first, 1.0, 0.0).astype(BF)


def kernel(
    ny, nr,
    src, tgt, hubf, ws, wn, bias, picks, et, es, hs, ht,
    vout, hout,
    col, idb, xbuf, table, hubp, hubr, tsel, cnt, cacc, dacc, acc, own,
    ring_s, ring_r, ids_s, ids_r, x_s, x_r, tab_s, tab_r, part_s, part_r,
):
    nz, nx, group = NZ, NX, ny * nr
    rows, width = col.shape[1], col.shape[2]
    cap = picks.shape[1]
    block = nx * cap
    mine = hubf.shape[0]
    hubs = group * mine
    base = nz * block
    chunk = rows // CHUNKS
    half = nz // 2
    edges = et.shape[1]
    part = edges // 2
    pair = 2 * LANES

    blk = lax.axis_index("blk")
    z, x = lax.div(blk, nx), lax.rem(blk, nx)
    m = lax.axis_index("hub") * nr + lax.axis_index("rep")

    def at_z(step):
        return lax.rem(z + step + nz, nz)

    def to_x(dx):
        return {"blk": z * nx + lax.rem(x + dx, nx)}

    def to_member(k):
        other = lax.rem(m + k, group)
        return {"hub": lax.div(other, nr), "rep": lax.rem(other, nr)}

    def ring_next(way):
        return {"blk": at_z(1 if way == 0 else -1) * nx + x}

    def remote(a, b, s, r, device):
        return pltpu.make_async_remote_copy(
            src_ref=a, dst_ref=b, send_sem=s, recv_sem=r, device_id=device, device_id_type=MESH
        )

    def ring_copy(way, owner, step, c):
        at = col.at[owner, pl.ds(c * chunk, chunk), :]
        return remote(at, at, ring_s.at[way, step - 1, c], ring_r.at[way, step - 1, c], ring_next(way))

    def ids_copy(way, owner, step):
        at = idb.at[owner]
        return remote(at, at, ids_s.at[way, step - 1], ids_r.at[way, step - 1], ring_next(way))

    def x_copy(owner, dx):
        there = lax.rem(x + dx, nx)
        a = xbuf.at[owner, pl.ds(pl.multiple_of(there * cap, cap), cap), :]
        b = table.at[pl.ds(pl.multiple_of((owner * nx + x) * cap, cap), cap), :]
        return remote(a, b, x_s.at[dx - 1, owner], x_r.at[dx - 1, owner], to_x(dx))

    def tab_copy(k):
        at = table.at[pl.ds(pl.multiple_of(base + m * mine, mine), mine), :]
        return remote(at, at, tab_s.at[k - 1], tab_r.at[k - 1], to_member(k))

    def part_copy(k):
        other = lax.rem(m + k, group)
        a = hubp.at[pl.ds(pl.multiple_of(other * mine, mine), mine), :]
        return remote(a, hubr.at[m], part_s.at[k - 1], part_r.at[k - 1], to_member(k))

    barrier = pltpu.get_barrier_semaphore()
    for way in (0, 1):
        pl.semaphore_signal(barrier, inc=1, device_id=ring_next(way), device_id_type=MESH)
    for dx in range(1, nx):
        pl.semaphore_signal(barrier, inc=1, device_id=to_x(dx), device_id_type=MESH)
    for k in range(1, group):
        pl.semaphore_signal(barrier, inc=1, device_id=to_member(k), device_id_type=MESH)

    col[z] = dot(src[...], wn[...], (1, 0)).astype(BF)
    table[pl.ds(pl.multiple_of(base + m * mine, mine), mine), :] = dot(hubf[...], wn[...], (1, 0)).astype(BF)
    ids = [picks[pl.ds(j, nz, stride=nx), :] for j in range(nx)]
    idb[z] = jnp.concatenate(ids, axis=1).astype(F32).astype(BF)

    pl.semaphore_wait(barrier, 2 + (nx - 1) + (group - 1))

    for way in (0, 1):
        ids_copy(way, z, 1).start()
    for c in range(CHUNKS):
        for way in (0, 1):
            ring_copy(way, z, 1, c).start()
    for k in range(1, group):
        tab_copy(k).start()

    def choose(owner):
        tile = idb[owner].astype(F32)
        which = lax.broadcasted_iota(jnp.int32, tile.shape, 0)
        row = jnp.sum(jnp.where(which == z, tile, 0.0), axis=0, keepdims=True)
        pick = one_hot(row.astype(jnp.int32), 0, rows)
        xbuf[owner] = dot(pick, col[owner], (0, 0)).astype(BF)
        keep = xbuf[owner, pl.ds(pl.multiple_of(x * cap, cap), cap), :]
        table[pl.ds(pl.multiple_of((owner * nx + x) * cap, cap), cap), :] = keep

    def hand_out(owner):
        for dx in range(1, nx):
            x_copy(owner, dx).start()

    def count_half(n, h):
        marks = one_hot(es[:, h * part : (h + 1) * part], n * pair, pair)
        got = dot(tsel[:, h * part : (h + 1) * part], marks, (1, 1))
        if h == 0:
            cacc[...] = got
            return
        got = got + cacc[...]
        dacc[...] += got[:, :LANES] + got[:, LANES:]
        high = jnp.floor(got * (1.0 / 256.0))
        low = got - 256.0 * high
        for j in range(2):
            lanes = slice(j * LANES, (j + 1) * LANES)
            cnt[2 * n + j, :, :LANES] = low[:, lanes].astype(BF)
            cnt[2 * n + j, :, LANES:] = high[:, lanes].astype(BF)

    def add_slab(slab):
        start = slab * LANES if isinstance(slab, int) else pl.multiple_of(slab * LANES, LANES)
        t = table[pl.ds(start, LANES), :]
        both = jnp.concatenate([t, (t.astype(F32) * 256.0).astype(BF)], axis=0)
        acc[...] += dot(cnt[slab], both, (1, 0))

    def take(owner):
        for dx in range(1, nx):
            x_copy(owner, dx).wait_recv()
        add_slab(owner)

    def pass_on(step, c):
        for way in (0, 1):
            owner = at_z(-step if way == 0 else step)
            if c == 0:
                ids_copy(way, owner, step).wait_recv()
                ids_copy(way, owner, step + 1).start()
            ring_copy(way, owner, step, c).wait_recv()
            ring_copy(way, owner, step + 1, c).start()

    hub_rows = dot(one_hot(hs[...], 0, rows), col[z], (0, 0)).astype(BF)
    marks = one_hot(ht[...], 0, hubs)
    hubp[:, :width] = dot(marks, hub_rows, (1, 0))
    hubp[:, width:] = jnp.broadcast_to(
        jnp.sum(marks.astype(F32), axis=1, keepdims=True), (hubs, LANES)
    )
    choose(z)
    tsel[...] = one_hot(et[...], 0, tgt.shape[0])
    acc[...] = jnp.zeros_like(acc)
    dacc[...] = jnp.zeros_like(dacc)
    for k in range(1, group):
        part_copy(k).start()
    hand_out(z)
    count_half(nz // 2, 0)
    count_half(nz // 2, 1)

    def early(step, carry):
        for c in range(CHUNKS):
            pass_on(step, c)
            if c == CHUNKS - 1:
                choose(at_z(-step))
                choose(at_z(step))
            count_half(2 * (step - 1) + c // 2, c % 2)
        hand_out(at_z(-step))
        hand_out(at_z(step))
        return carry

    lax.fori_loop(1, half // 2 + 1, early, 0)

    def late(step, carry):
        for c in range(CHUNKS):
            pass_on(step, c)
            if c == CHUNKS - 1:
                choose(at_z(-step))
                choose(at_z(step))
            back = 2 * (step - half // 2 - 1) + 1 + c // 2
            take(at_z(-back if c % 2 == 0 else back))
        hand_out(at_z(-step))
        hand_out(at_z(step))
        return carry

    lax.fori_loop(half // 2 + 1, half - 1, late, 0)

    step = half - 1
    for c in range(CHUNKS):
        for way in (0, 1):
            owner = at_z(-step if way == 0 else step)
            if c == 0:
                ids_copy(way, owner, step).wait_recv()
                if way == 0:
                    ids_copy(way, owner, half).start()
            ring_copy(way, owner, step, c).wait_recv()
            if way == c // (CHUNKS // 2):
                ring_copy(way, owner, half, c).start()
        if c == 0:
            own[...] = dot(tgt[...], ws[...], (1, 0)) + bias[...]
        if c == 1:
            take(z)
        if c == 2:
            for k in range(1, group):
                tab_copy(k).wait_recv()
            add_slab(nz)
            add_slab(nz + 1)
    choose(at_z(-step))
    choose(at_z(step))
    for k in range(1, group):
        part_copy(k).wait_recv()
    total = hubp[pl.ds(pl.multiple_of(m * mine, mine), mine), :]
    for k in range(1, group):
        total = total + hubr[lax.rem(m + k, group)]
    fed = total[:, :width] / jnp.maximum(total[:, width : width + 1], 1.0)
    mean = dot(hubf[...], ws[...], (1, 0)) + fed + bias[...]
    hout[...] = jnp.maximum(mean, 0.0).astype(hout.dtype)
    hand_out(at_z(-step))
    hand_out(at_z(step))
    take(at_z(-(half - 3)))
    take(at_z(half - 3))

    far = at_z(half)
    ids_copy(0, far, half).wait_recv()
    for c in range(CHUNKS):
        ring_copy(c // (CHUNKS // 2), far, half, c).wait_recv()
    choose(far)
    take(at_z(-(half - 2)))
    hand_out(far)
    take(at_z(half - 2))
    take(at_z(-step))
    take(at_z(step))
    scale = 1.0 / jnp.maximum(jnp.sum(dacc[...], axis=1, keepdims=True), 1.0)
    take(far)
    vout[...] = jnp.maximum(own[...] + acc[...] * scale, 0.0).astype(vout.dtype)

    def sent(step, carry):
        for way in (0, 1):
            ids_copy(way, z, step).wait_send()
            for c in range(CHUNKS):
                ring_copy(way, z, step, c).wait_send()
        return carry

    lax.fori_loop(1, half, sent, 0)
    ids_copy(0, z, half).wait_send()
    for c in range(CHUNKS):
        ring_copy(c // (CHUNKS // 2), z, half, c).wait_send()

    def sent_x(owner, carry):
        for dx in range(1, nx):
            x_copy(owner, dx).wait_send()
        return carry

    lax.fori_loop(0, nz, sent_x, 0)
    for k in range(1, group):
        tab_copy(k).wait_send()
        part_copy(k).wait_send()


def on_device(
    source_feats,
    target_feats,
    hub_feats,
    weight_self,
    weight_neigh,
    bias_vector,
    send_rows,
    edge_target,
    edge_slot,
    hub_source,
    hub_target,
):
    ny, nr = lax.axis_size("hub"), lax.axis_size("rep")
    rows, width = source_feats.shape[0], weight_neigh.shape[1]
    targets, mine, cap = target_feats.shape[0], hub_feats.shape[0], send_rows.shape[2]
    group = ny * nr
    hubs = group * mine
    slots = NZ * NX * cap + hubs
    edges = edge_target.shape[1]
    half = NZ // 2
    dma = pltpu.SemaphoreType.DMA
    vmem = pl.BlockSpec(memory_space=pltpu.VMEM)
    return pl.pallas_call(
        functools.partial(kernel, ny, nr),
        out_shape=(
            jax.ShapeDtypeStruct((targets, width), BF),
            jax.ShapeDtypeStruct((mine, width), BF),
        ),
        in_specs=[vmem] * 11,
        out_specs=(vmem, vmem),
        scratch_shapes=[
            pltpu.VMEM((NZ, rows, width), BF),
            pltpu.VMEM((NZ, NZ, NX * cap), BF),
            pltpu.VMEM((NZ, NX * cap, width), BF),
            pltpu.VMEM((slots, width), BF),
            pltpu.VMEM((hubs, width + LANES), F32),
            pltpu.VMEM((group, mine, width + LANES), F32),
            pltpu.VMEM((targets, edges), BF),
            pltpu.VMEM((slots // LANES, targets, 2 * LANES), BF),
            pltpu.VMEM((targets, 2 * LANES), F32),
            pltpu.VMEM((targets, LANES), F32),
            pltpu.VMEM((targets, width), F32),
            pltpu.VMEM((targets, width), F32),
            dma((2, half, CHUNKS)),
            dma((2, half, CHUNKS)),
            dma((2, half)),
            dma((2, half)),
            dma((NX - 1, NZ)),
            dma((NX - 1, NZ)),
            dma((group - 1,)),
            dma((group - 1,)),
            dma((group - 1,)),
            dma((group - 1,)),
        ],
        compiler_params=pltpu.CompilerParams(
            collective_id=0, has_side_effects=True, vmem_limit_bytes=40 * 1024 * 1024
        ),
    )(
        source_feats,
        target_feats,
        hub_feats,
        weight_self,
        weight_neigh,
        bias_vector.reshape(1, width),
        send_rows[0],
        edge_target,
        edge_slot,
        hub_source,
        hub_target,
    )


def solution(mesh):
    rows = P(("blk", "hub", "rep"), None)
    in_specs = (
        rows, rows, rows, P(), P(), P(),
        P(("blk", "hub", "rep"), None, None),
        rows, rows, rows, rows,
    )
    return jax.shard_map(
        on_device, mesh=mesh, in_specs=in_specs, out_specs=(rows, rows), check_vma=False
    )
```

```python
import functools

import jax
import jax.numpy as jnp
from jax import lax
from jax.experimental import pallas as pl
from jax.experimental.pallas import tpu as pltpu
from jax.sharding import PartitionSpec as P

MESH = pl.DeviceIdType.MESH
NZ, NX = 16, 4
CHUNKS = 4
RING = 5
LANES = 128
BF, F32, F8 = jnp.bfloat16, jnp.float32, jnp.float8_e4m3fn


def dot(a, b, contract):
    return lax.dot_general(a, b, ((contract[:1], contract[1:]), ((), ())), preferred_element_type=F32)


def one_hot(ids, first, count):
    n = ids.shape[1]
    parts = []
    rows = lax.broadcasted_iota(jnp.int32, (256, LANES), 0).astype(F32).astype(BF)
    rows = jnp.concatenate([rows] * (n // LANES), axis=1)
    for at in range(0, count, 256):
        near = jnp.broadcast_to(ids - (first + at), (16, n)).astype(F32).astype(BF)
        near = jnp.concatenate([near] * 16, axis=0)
        parts.append(jnp.where(rows == near, BF(1.0), BF(0.0)))
    return parts[0] if len(parts) == 1 else jnp.concatenate(parts, axis=0)


def kernel(
    ny, nr,
    src_h, wn_h, hubf_h, picks_h, hs_h, ht_h, et_h, es_h, tgt_h, ws_h, bias_h,
    vout, hout,
    src, wn, hubf, picks, hs, ht, et, es, tgt, ws, bias, turned,
    col, idb, xbuf, table, hubp, hubr, tsel, cnt, cacc, dacc, acc, own, far_buf,
    ring_s, ring_r, ids_s, ids_r, x_s, x_r, tab_s, tab_r, part_s, part_r, far_s, far_r, in_s,
):
    nz, nx, group = NZ, NX, ny * nr
    rows, width = col.shape[1], col.shape[2]
    cap = picks.shape[0]
    block = nx * cap
    mine = hubf.shape[0]
    hubs = group * mine
    base = nz * block
    chunk = rows // CHUNKS
    half = nz // 2
    edges = et.shape[1]
    part = edges // 2
    pair = 2 * LANES

    blk = lax.axis_index("blk")
    z, x = lax.div(blk, nx), lax.rem(blk, nx)
    m = lax.axis_index("hub") * nr + lax.axis_index("rep")

    def at_z(step):
        return lax.rem(z + step + nz, nz)

    def to_x(dx):
        return {"blk": z * nx + lax.rem(x + dx, nx)}

    def to_member(k):
        other = lax.rem(m + k, group)
        return {"hub": lax.div(other, nr), "rep": lax.rem(other, nr)}

    def ring_next(way):
        return {"blk": at_z(1 if way == 0 else -1) * nx + x}

    def remote(a, b, s, r, device):
        return pltpu.make_async_remote_copy(
            src_ref=a, dst_ref=b, send_sem=s, recv_sem=r, device_id=device, device_id_type=MESH
        )

    def ring_copy(way, owner, step, c):
        at = col.at[owner, pl.ds(c * chunk, chunk), :]
        return remote(at, at, ring_s.at[way, step - 1, c], ring_r.at[way, step - 1, c], ring_next(way))

    def ids_copy(way, owner, step):
        at = idb.at[owner]
        return remote(at, at, ids_s.at[way, step - 1], ids_r.at[way, step - 1], ring_next(way))

    def far_copy(way, k, owner):
        at = k - RING - 1
        first, last = (0, block) if k < half else (way * block // 2, (way + 1) * block // 2)
        there = at_z(k - RING if way == 0 else RING - k)
        return remote(
            far_buf.at[way, at, pl.ds(first, last - first), :],
            xbuf.at[owner, pl.ds(first, last - first), :],
            far_s.at[way, at],
            far_r.at[way, at],
            {"blk": there * nx + x},
        )

    def x_copy(owner, dx):
        there = lax.rem(x + dx, nx)
        a = xbuf.at[owner, pl.ds(pl.multiple_of(there * cap, cap), cap), :]
        b = table.at[pl.ds(pl.multiple_of((owner * nx + x) * cap, cap), cap), :]
        return remote(a, b, x_s.at[dx - 1, owner], x_r.at[dx - 1, owner], to_x(dx))

    def tab_copy(k):
        at = table.at[pl.ds(pl.multiple_of(base + m * mine, mine), mine), :]
        return remote(at, at, tab_s.at[k - 1], tab_r.at[k - 1], to_member(k))

    def part_copy(k):
        other = lax.rem(m + k, group)
        a = hubp.at[pl.ds(pl.multiple_of(other * mine, mine), mine), :]
        return remote(a, hubr.at[m], part_s.at[k - 1], part_r.at[k - 1], to_member(k))

    inputs = (
        (src_h, src), (wn_h, wn), (hubf_h, hubf), (picks_h, picks), (hs_h, hs), (ht_h, ht),
        (et_h, et), (es_h, es), (tgt_h, tgt), (ws_h, ws), (bias_h, bias),
    )
    loads = [pltpu.make_async_copy(a, b, in_s.at[i]) for i, (a, b) in enumerate(inputs)]
    for load in loads:
        load.start()

    barrier = pltpu.get_barrier_semaphore()
    reach = half - RING
    for k in range(1, reach + 1):
        for there in (at_z(k), at_z(-k)):
            pl.semaphore_signal(barrier, inc=1, device_id={"blk": there * nx + x}, device_id_type=MESH)
    for dx in range(1, nx):
        pl.semaphore_signal(barrier, inc=1, device_id=to_x(dx), device_id_type=MESH)
    for k in range(1, group):
        pl.semaphore_signal(barrier, inc=1, device_id=to_member(k), device_id_type=MESH)

    for load in loads[:4]:
        load.wait()
    col[z] = dot(src[...], wn[...], (1, 0)).astype(BF)
    table[pl.ds(pl.multiple_of(base + m * mine, mine), mine), :] = dot(hubf[...], wn[...], (1, 0)).astype(BF)
    turned[...] = picks[...].astype(F32).T
    ids = [turned[pl.ds(j, nz, stride=nx), :] for j in range(nx)]
    idb[z] = jnp.concatenate(ids, axis=1).astype(BF)

    pl.semaphore_wait(barrier, 2 * reach + (nx - 1) + (group - 1))

    for c in range(CHUNKS):
        for way in (0, 1):
            ring_copy(way, z, 1, c).start()
    for way in (0, 1):
        ids_copy(way, z, 1).start()
    for k in range(1, group):
        tab_copy(k).start()

    def chosen(owner, place):
        tile = idb[owner].astype(F32)
        which = lax.broadcasted_iota(jnp.int32, tile.shape, 0)
        row = jnp.sum(jnp.where(which == place, tile, 0.0), axis=0, keepdims=True)
        pick = one_hot(row.astype(jnp.int32), 0, rows)
        return dot(pick, col[owner], (0, 0)).astype(BF)

    def keep(owner):
        mine_too = xbuf[owner, pl.ds(pl.multiple_of(x * cap, cap), cap), :]
        table[pl.ds(pl.multiple_of((owner * nx + x) * cap, cap), cap), :] = mine_too

    def choose(owner):
        xbuf[owner] = chosen(owner, z)
        keep(owner)

    def hand_out(owner):
        for dx in range(1, nx):
            x_copy(owner, dx).start()

    def count_half(n, h):
        marks = one_hot(es[:, h * part : (h + 1) * part], n * pair, pair).astype(F8)
        got = dot(tsel[:, h * part : (h + 1) * part], marks, (1, 1))
        if h == 0:
            cacc[...] = got
            return
        got = got + cacc[...]
        dacc[...] += got[:, :LANES] + got[:, LANES:]
        high = jnp.floor(got * (1.0 / 256.0))
        low = got - 256.0 * high
        for j in range(2):
            lanes = slice(j * LANES, (j + 1) * LANES)
            cnt[2 * n + j, :, :LANES] = low[:, lanes].astype(BF)
            cnt[2 * n + j, :, LANES:] = high[:, lanes].astype(BF)

    def add_slab(slab):
        start = slab * LANES if isinstance(slab, int) else pl.multiple_of(slab * LANES, LANES)
        t = table[pl.ds(start, LANES), :]
        both = jnp.concatenate([t, (t.astype(F32) * 256.0).astype(BF)], axis=0)
        acc[...] += dot(cnt[slab], both, (1, 0))

    def take(owner):
        for dx in range(1, nx):
            x_copy(owner, dx).wait_recv()
        add_slab(owner)

    def pass_on(step, c):
        for way in (0, 1):
            owner = at_z(-step if way == 0 else step)
            ring_copy(way, owner, step, c).wait_recv()
            ring_copy(way, owner, step + 1, c).start()
            if c == CHUNKS - 1:
                ids_copy(way, owner, step).wait_recv()
                ids_copy(way, owner, step + 1).start()

    for load in loads[4:]:
        load.wait()
    hub_rows = dot(one_hot(hs[...], 0, rows), col[z], (0, 0)).astype(BF)
    marks = one_hot(ht[...], 0, hubs)
    hubp[:, :width] = dot(marks, hub_rows, (1, 0))
    hubp[:, width:] = jnp.broadcast_to(
        jnp.sum(marks.astype(F32), axis=1, keepdims=True), (hubs, LANES)
    )
    choose(z)
    tsel[...] = one_hot(et[...], 0, tgt.shape[0]).astype(F8)
    acc[...] = jnp.zeros_like(acc)
    dacc[...] = jnp.zeros_like(dacc)
    for k in range(1, group):
        part_copy(k).start()
    hand_out(z)
    count_half(nz // 2, 0)
    count_half(nz // 2, 1)

    def early(step, carry):
        for c in range(CHUNKS):
            pass_on(step, c)
            if c == CHUNKS - 1:
                choose(at_z(-step))
                choose(at_z(step))
            count_half(2 * (step - 1) + c // 2, c % 2)
        hand_out(at_z(-step))
        hand_out(at_z(step))
        return carry

    lax.fori_loop(1, half // 2 + 1, early, 0)

    for c in range(CHUNKS):
        for way in (0, 1):
            owner = at_z(-RING if way == 0 else RING)
            ring_copy(way, owner, RING, c).wait_recv()
            if c == CHUNKS - 1:
                ids_copy(way, owner, RING).wait_recv()
        if c == 0:
            own[...] = dot(tgt[...], ws[...], (1, 0)) + bias[...]
        if c == 1:
            for k in range(1, group):
                tab_copy(k).wait_recv()
            add_slab(nz)
            add_slab(nz + 1)
            take(z)
        if c == 2:
            for back in (1, 2):
                take(at_z(-back))
                take(at_z(back))
    beyond = range(half, RING, -1)
    for k in beyond:
        for way in (0, 1):
            owner = at_z(-RING if way == 0 else RING)
            far_buf[way, k - RING - 1] = chosen(owner, at_z(k - RING if way == 0 else RING - k))
    for k in beyond:
        for way in (0, 1):
            far_copy(way, k, at_z(-RING if way == 0 else RING)).start()
    choose(at_z(-RING))
    choose(at_z(RING))
    for k in range(1, group):
        part_copy(k).wait_recv()
    total = hubp[pl.ds(pl.multiple_of(m * mine, mine), mine), :]
    for k in range(1, group):
        total = total + hubr[lax.rem(m + k, group)]
    hand_out(at_z(-RING))
    hand_out(at_z(RING))
    fed = total[:, :width] / jnp.maximum(total[:, width : width + 1], 1.0)
    mean = dot(hubf[...], ws[...], (1, 0)) + fed + bias[...]
    hout[...] = jnp.maximum(mean, 0.0).astype(hout.dtype)
    for back in range(3, RING):
        take(at_z(-back))
        take(at_z(back))

    for k in range(RING + 1, half + 1):
        for way in (0, 1):
            owner = at_z(-k if way == 0 else k)
            far_copy(way, k, owner).wait_recv()
            if k < half:
                hand_out(owner)
                keep(owner)
    hand_out(at_z(half))
    keep(at_z(half))
    for back in range(RING, half):
        take(at_z(-back))
        take(at_z(back))
    far = at_z(half)
    scale = 1.0 / jnp.maximum(jnp.sum(dacc[...], axis=1, keepdims=True), 1.0)
    take(far)
    vout[...] = jnp.maximum(own[...] + acc[...] * scale, 0.0).astype(vout.dtype)

    def sent(step, carry):
        for way in (0, 1):
            ids_copy(way, z, step).wait_send()
            for c in range(CHUNKS):
                ring_copy(way, z, step, c).wait_send()
        return carry

    lax.fori_loop(1, RING + 1, sent, 0)
    for k in beyond:
        for way in (0, 1):
            far_copy(way, k, z).wait_send()

    def sent_x(owner, carry):
        for dx in range(1, nx):
            x_copy(owner, dx).wait_send()
        return carry

    lax.fori_loop(0, nz, sent_x, 0)
    for k in range(1, group):
        tab_copy(k).wait_send()
        part_copy(k).wait_send()


def on_device(
    source_feats,
    target_feats,
    hub_feats,
    weight_self,
    weight_neigh,
    bias_vector,
    send_rows,
    edge_target,
    edge_slot,
    hub_source,
    hub_target,
):
    ny, nr = lax.axis_size("hub"), lax.axis_size("rep")
    rows, width = source_feats.shape[0], weight_neigh.shape[1]
    targets, mine, cap = target_feats.shape[0], hub_feats.shape[0], send_rows.shape[2]
    group = ny * nr
    hubs = group * mine
    slots = NZ * NX * cap + hubs
    edges = edge_target.shape[1]
    half = NZ // 2
    operands = (
        source_feats,
        weight_neigh,
        hub_feats,
        send_rows[0].T,
        hub_source,
        hub_target,
        edge_target,
        edge_slot,
        target_feats,
        weight_self,
        bias_vector.reshape(1, width),
    )
    dma = pltpu.SemaphoreType.DMA
    vmem = pl.BlockSpec(memory_space=pltpu.VMEM)
    return pl.pallas_call(
        functools.partial(kernel, ny, nr),
        out_shape=(
            jax.ShapeDtypeStruct((targets, width), BF),
            jax.ShapeDtypeStruct((mine, width), BF),
        ),
        in_specs=[pl.BlockSpec(memory_space=pltpu.HBM)] * 11,
        out_specs=(vmem, vmem),
        scratch_shapes=[pltpu.VMEM(a.shape, a.dtype) for a in operands]
        + [
            pltpu.VMEM((NZ * NX, cap), F32),
            pltpu.VMEM((NZ, rows, width), BF),
            pltpu.VMEM((NZ, NZ, NX * cap), BF),
            pltpu.VMEM((NZ, NX * cap, width), BF),
            pltpu.VMEM((slots, width), BF),
            pltpu.VMEM((hubs, width + LANES), F32),
            pltpu.VMEM((group, mine, width + LANES), F32),
            pltpu.VMEM((targets, edges), F8),
            pltpu.VMEM((slots // LANES, targets, 2 * LANES), BF),
            pltpu.VMEM((targets, 2 * LANES), F32),
            pltpu.VMEM((targets, LANES), F32),
            pltpu.VMEM((targets, width), F32),
            pltpu.VMEM((targets, width), F32),
            pltpu.VMEM((2, half - RING, NX * cap, width), BF),
            dma((2, RING, CHUNKS)),
            dma((2, RING, CHUNKS)),
            dma((2, RING)),
            dma((2, RING)),
            dma((NX - 1, NZ)),
            dma((NX - 1, NZ)),
            dma((group - 1,)),
            dma((group - 1,)),
            dma((group - 1,)),
            dma((group - 1,)),
            dma((2, half - RING)),
            dma((2, half - RING)),
            dma((len(operands),)),
        ],
        compiler_params=pltpu.CompilerParams(
            collective_id=0, has_side_effects=True, vmem_limit_bytes=67043328
        ),
    )(*operands)


def solution(mesh):
    rows = P(("blk", "hub", "rep"), None)
    in_specs = (
        rows, rows, rows, P(), P(), P(),
        P(("blk", "hub", "rep"), None, None),
        rows, rows, rows, rows,
    )
    return jax.shard_map(
        on_device, mesh=mesh, in_specs=in_specs, out_specs=(rows, rows), check_vma=False
    )
```

```python
import functools

import jax
import jax.numpy as jnp
from jax import lax
from jax.experimental import pallas as pl
from jax.experimental.pallas import tpu as pltpu
from jax.sharding import PartitionSpec as P

MESH = pl.DeviceIdType.MESH
NZ, NX = 16, 4
CHUNKS = 4
RING = 6
LANES = 128
DIRECT = (7, 8)
BF, F32, F8 = jnp.bfloat16, jnp.float32, jnp.float8_e4m3fn


def dot(a, b, contract):
    return lax.dot_general(a, b, ((contract[:1], contract[1:]), ((), ())), preferred_element_type=F32)


def one_hot(ids, first, count):
    n = ids.shape[1]
    parts = []
    rows = lax.broadcasted_iota(jnp.int32, (256, LANES), 0).astype(F32).astype(BF)
    rows = jnp.concatenate([rows] * (n // LANES), axis=1)
    for at in range(0, count, 256):
        near = jnp.broadcast_to(ids - (first + at), (16, n)).astype(F32).astype(BF)
        near = jnp.concatenate([near] * 16, axis=0)
        parts.append(jnp.where(rows == near, BF(1.0), BF(0.0)))
    return parts[0] if len(parts) == 1 else jnp.concatenate(parts, axis=0)


def kernel(
    ny, nr,
    src_h, wn_h, hubf_h, picks_h, hs_h, ht_h, et_h, es_h, tgt_h, ws_h, bias_h,
    vout, hout,
    src, wn, hubf, picks, hs, ht, et, es, tgt, ws, bias, turned,
    col, idb, xbuf, table, hubp, hubr, tsel, cnt, cacc, dacc, acc, own, far_buf,
    ring_s, ring_r, ids_s, ids_r, x_s, x_r, tab_s, tab_r, part_s, part_r, far_s, far_r, end_s, end_r, in_s,
):
    nz, nx, group = NZ, NX, ny * nr
    rows, width = col.shape[1], col.shape[2]
    cap = picks.shape[0]
    block = nx * cap
    mine = hubf.shape[0]
    hubs = group * mine
    base = nz * block
    chunk = rows // CHUNKS
    half = nz // 2
    edges = et.shape[1]
    part = edges // 2
    pair = 2 * LANES

    blk = lax.axis_index("blk")
    z, x = lax.div(blk, nx), lax.rem(blk, nx)
    m = lax.axis_index("hub") * nr + lax.axis_index("rep")

    def at_z(step):
        return lax.rem(z + step + nz, nz)

    def to_x(dx):
        return {"blk": z * nx + lax.rem(x + dx, nx)}

    def to_member(k):
        other = lax.rem(m + k, group)
        return {"hub": lax.div(other, nr), "rep": lax.rem(other, nr)}

    def ring_next(way):
        return {"blk": at_z(1 if way == 0 else -1) * nx + x}

    def remote(a, b, s, r, device):
        return pltpu.make_async_remote_copy(
            src_ref=a, dst_ref=b, send_sem=s, recv_sem=r, device_id=device, device_id_type=MESH
        )

    def ring_copy(way, owner, step, c):
        at = col.at[owner, pl.ds(c * chunk, chunk), :]
        return remote(at, at, ring_s.at[way, step - 1, c], ring_r.at[way, step - 1, c], ring_next(way))

    def ids_copy(way, owner, step):
        at = idb.at[owner]
        return remote(at, at, ids_s.at[way, step - 1], ids_r.at[way, step - 1], ring_next(way))

    def far_copy(way, k, owner):
        at = k - RING - 1
        first, last = (0, block) if k < half else (way * block // 2, (way + 1) * block // 2)
        there = at_z(k - RING if way == 0 else RING - k)
        return remote(
            far_buf.at[way, at, pl.ds(first, last - first), :],
            xbuf.at[owner, pl.ds(first, last - first), :],
            far_s.at[way, at],
            far_r.at[way, at],
            {"blk": there * nx + x},
        )

    def end_places(way, k):
        return range(nx) if k < half else range(way * nx // 2, (way + 1) * nx // 2)

    def end_copy(way, k, owner, sender, place):
        at = k - RING - 1
        there = lax.rem(z + nz + (k - RING) - 2 * (k - RING) * way, nz)
        return remote(
            far_buf.at[way, at, pl.ds(place * cap, cap), :],
            table.at[pl.ds(pl.multiple_of((owner * nx + sender) * cap, cap), cap), :],
            end_s.at[way, at, place],
            end_r.at[way, at, sender],
            {"blk": there * nx + place},
        )

    def end_wait(way, k, owner):
        for sender in range(nx):
            end_copy(way, k, owner, sender, 0).wait_recv()

    def x_copy(owner, dx):
        there = lax.rem(x + dx, nx)
        a = xbuf.at[owner, pl.ds(pl.multiple_of(there * cap, cap), cap), :]
        b = table.at[pl.ds(pl.multiple_of((owner * nx + x) * cap, cap), cap), :]
        return remote(a, b, x_s.at[dx - 1, owner], x_r.at[dx - 1, owner], to_x(dx))

    def tab_copy(k):
        at = table.at[pl.ds(pl.multiple_of(base + m * mine, mine), mine), :]
        return remote(at, at, tab_s.at[k - 1], tab_r.at[k - 1], to_member(k))

    def part_copy(k):
        other = lax.rem(m + k, group)
        a = hubp.at[pl.ds(pl.multiple_of(other * mine, mine), mine), :]
        return remote(a, hubr.at[m], part_s.at[k - 1], part_r.at[k - 1], to_member(k))

    inputs = (
        (src_h, src), (wn_h, wn), (hubf_h, hubf), (picks_h, picks), (hs_h, hs), (ht_h, ht),
        (et_h, et), (es_h, es), (tgt_h, tgt), (ws_h, ws), (bias_h, bias),
    )
    loads = [pltpu.make_async_copy(a, b, in_s.at[i]) for i, (a, b) in enumerate(inputs)]
    for load in loads:
        load.start()

    barrier = pltpu.get_barrier_semaphore()
    reach = half - RING
    near = [(there, j) for k in range(1, reach + 1) if RING + k in DIRECT and k < reach
            for there in (at_z(k), at_z(-k)) for j in range(nx)]
    near += [(there, x) for k in range(1, reach + 1) if RING + k not in DIRECT for there in (at_z(k), at_z(-k))]
    if RING > 1 and RING + 1 in DIRECT and reach == 1:
        near += [(at_z(1), x), (at_z(-1), x)]
    if half in DIRECT:
        near += [(lax.rem(z + nz - reach + 2 * reach * lax.div(x, nx // 2), nz), j) for j in range(nx)]
    for there, j in near:
        pl.semaphore_signal(barrier, inc=1, device_id={"blk": there * nx + j}, device_id_type=MESH)
    for dx in range(1, nx):
        pl.semaphore_signal(barrier, inc=1, device_id=to_x(dx), device_id_type=MESH)
    for k in range(1, group):
        pl.semaphore_signal(barrier, inc=1, device_id=to_member(k), device_id_type=MESH)

    for load in loads[:4]:
        load.wait()
    col[z] = dot(src[...], wn[...], (1, 0)).astype(BF)
    table[pl.ds(pl.multiple_of(base + m * mine, mine), mine), :] = dot(hubf[...], wn[...], (1, 0)).astype(BF)
    turned[...] = picks[...].astype(F32).T
    ids = [turned[pl.ds(j, nz, stride=nx), :] for j in range(nx)]
    idb[z] = jnp.concatenate(ids, axis=1).astype(BF)

    pl.semaphore_wait(barrier, len(near) + (nx - 1) + (group - 1))

    for c in range(CHUNKS):
        for way in (0, 1):
            ring_copy(way, z, 1, c).start()
    for way in (0, 1):
        ids_copy(way, z, 1).start()
    for k in range(1, group):
        tab_copy(k).start()

    def chosen(owner, place):
        tile = idb[owner].astype(F32)
        which = lax.broadcasted_iota(jnp.int32, tile.shape, 0)
        row = jnp.sum(jnp.where(which == place, tile, 0.0), axis=0, keepdims=True)
        pick = one_hot(row.astype(jnp.int32), 0, rows)
        return dot(pick, col[owner], (0, 0)).astype(BF)

    def keep(owner):
        mine_too = xbuf[owner, pl.ds(pl.multiple_of(x * cap, cap), cap), :]
        table[pl.ds(pl.multiple_of((owner * nx + x) * cap, cap), cap), :] = mine_too

    def choose(owner):
        xbuf[owner] = chosen(owner, z)
        keep(owner)

    def hand_out(owner):
        for dx in range(1, nx):
            x_copy(owner, dx).start()

    def count_half(n, h):
        marks = one_hot(es[:, h * part : (h + 1) * part], n * pair, pair).astype(F8)
        got = dot(tsel[:, h * part : (h + 1) * part], marks, (1, 1))
        if h == 0:
            cacc[...] = got
            return
        got = got + cacc[...]
        dacc[...] += got[:, :LANES] + got[:, LANES:]
        high = jnp.floor(got * (1.0 / 256.0))
        low = got - 256.0 * high
        for j in range(2):
            lanes = slice(j * LANES, (j + 1) * LANES)
            cnt[2 * n + j, :, :LANES] = low[:, lanes].astype(BF)
            cnt[2 * n + j, :, LANES:] = high[:, lanes].astype(BF)

    def add_slab(slab):
        start = slab * LANES if isinstance(slab, int) else pl.multiple_of(slab * LANES, LANES)
        t = table[pl.ds(start, LANES), :]
        both = jnp.concatenate([t, (t.astype(F32) * 256.0).astype(BF)], axis=0)
        acc[...] += dot(cnt[slab], both, (1, 0))

    def take(owner):
        for dx in range(1, nx):
            x_copy(owner, dx).wait_recv()
        add_slab(owner)

    def pass_on(step, c):
        for way in (0, 1):
            owner = at_z(-step if way == 0 else step)
            ring_copy(way, owner, step, c).wait_recv()
            ring_copy(way, owner, step + 1, c).start()
            if c == CHUNKS - 1:
                ids_copy(way, owner, step).wait_recv()
                ids_copy(way, owner, step + 1).start()

    for load in loads[4:]:
        load.wait()
    hub_rows = dot(one_hot(hs[...], 0, rows), col[z], (0, 0)).astype(BF)
    marks = one_hot(ht[...], 0, hubs)
    hubp[:, :width] = dot(marks, hub_rows, (1, 0))
    hubp[:, width:] = jnp.broadcast_to(
        jnp.sum(marks.astype(F32), axis=1, keepdims=True), (hubs, LANES)
    )
    choose(z)
    tsel[...] = one_hot(et[...], 0, tgt.shape[0]).astype(F8)
    acc[...] = jnp.zeros_like(acc)
    dacc[...] = jnp.zeros_like(dacc)
    for k in range(1, group):
        part_copy(k).start()
    hand_out(z)
    count_half(nz // 2, 0)
    count_half(nz // 2, 1)

    def early(step, carry):
        for c in range(CHUNKS):
            pass_on(step, c)
            if c == CHUNKS - 1:
                choose(at_z(-step))
                choose(at_z(step))
            count_half(2 * (step - 1) + c // 2, c % 2)
        hand_out(at_z(-step))
        hand_out(at_z(step))
        return carry

    lax.fori_loop(1, half // 2 + 1, early, 0)

    for step in range(half // 2 + 1, RING):
        for c in range(CHUNKS):
            pass_on(step, c)
        choose(at_z(-step))
        choose(at_z(step))
        take(z)
        hand_out(at_z(-step))
        hand_out(at_z(step))

    for c in range(CHUNKS):
        for way in (0, 1):
            owner = at_z(-RING if way == 0 else RING)
            ring_copy(way, owner, RING, c).wait_recv()
            if c == CHUNKS - 1:
                ids_copy(way, owner, RING).wait_recv()
        if c == 0:
            own[...] = dot(tgt[...], ws[...], (1, 0)) + bias[...]
        if c == 1:
            for k in range(1, group):
                tab_copy(k).wait_recv()
            add_slab(nz)
            add_slab(nz + 1)
        if c == 2:
            for back in (1, 2):
                take(at_z(-back))
                take(at_z(back))
    beyond = range(half, RING, -1)
    for k in beyond:
        for way in (0, 1):
            owner = at_z(-RING if way == 0 else RING)
            far_buf[way, k - RING - 1] = chosen(owner, at_z(k - RING if way == 0 else RING - k))
    for k in beyond:
        for way in (0, 1):
            owner = at_z(-RING if way == 0 else RING)
            if k not in DIRECT:
                far_copy(way, k, owner).start()
                continue
            for place in end_places(way, k):
                end_copy(way, k, owner, x, place).start()
    choose(at_z(-RING))
    choose(at_z(RING))
    for k in range(1, group):
        part_copy(k).wait_recv()
    total = hubp[pl.ds(pl.multiple_of(m * mine, mine), mine), :]
    for k in range(1, group):
        total = total + hubr[lax.rem(m + k, group)]
    hand_out(at_z(-RING))
    hand_out(at_z(RING))
    fed = total[:, :width] / jnp.maximum(total[:, width : width + 1], 1.0)
    mean = dot(hubf[...], ws[...], (1, 0)) + fed + bias[...]
    hout[...] = jnp.maximum(mean, 0.0).astype(hout.dtype)
    for back in range(3, RING):
        take(at_z(-back))
        take(at_z(back))

    for k in range(RING + 1, half + 1):
        for way in (0, 1):
            owner = at_z(-k if way == 0 else k)
            if k in DIRECT:
                continue
            far_copy(way, k, owner).wait_recv()
            if k < half or way == 1:
                hand_out(owner)
                keep(owner)
    take(at_z(-RING))
    take(at_z(RING))
    for k in sorted(range(RING + 1, half), key=lambda k: (k in DIRECT, k)):
        for way in (0, 1):
            owner = at_z(-k if way == 0 else k)
            if k in DIRECT:
                end_wait(way, k, owner)
                add_slab(owner)
            else:
                take(owner)
    far = at_z(half)
    scale = 1.0 / jnp.maximum(jnp.sum(dacc[...], axis=1, keepdims=True), 1.0)
    if half in DIRECT:
        end_wait(lax.div(x, nx // 2), half, far)
        add_slab(far)
    else:
        take(far)
    vout[...] = jnp.maximum(own[...] + acc[...] * scale, 0.0).astype(vout.dtype)

    def sent(step, carry):
        for way in (0, 1):
            ids_copy(way, z, step).wait_send()
            for c in range(CHUNKS):
                ring_copy(way, z, step, c).wait_send()
        return carry

    lax.fori_loop(1, RING + 1, sent, 0)
    for k in beyond:
        for way in (0, 1):
            if k not in DIRECT:
                far_copy(way, k, z).wait_send()
                continue
            for place in end_places(way, k):
                end_copy(way, k, z, x, place).wait_send()

    def sent_x(step, carry):
        owner = lax.rem(z + nz - handed + step, nz)
        for dx in range(1, nx):
            x_copy(owner, dx).wait_send()
        return carry

    handed = max(k for k in range(half + 1) if k not in DIRECT)
    lax.fori_loop(0, handed + min(handed, half - 1) + 1, sent_x, 0)
    for k in range(1, group):
        tab_copy(k).wait_send()
        part_copy(k).wait_send()


def on_device(
    source_feats,
    target_feats,
    hub_feats,
    weight_self,
    weight_neigh,
    bias_vector,
    send_rows,
    edge_target,
    edge_slot,
    hub_source,
    hub_target,
):
    ny, nr = lax.axis_size("hub"), lax.axis_size("rep")
    rows, width = source_feats.shape[0], weight_neigh.shape[1]
    targets, mine, cap = target_feats.shape[0], hub_feats.shape[0], send_rows.shape[2]
    group = ny * nr
    hubs = group * mine
    slots = NZ * NX * cap + hubs
    edges = edge_target.shape[1]
    half = NZ // 2
    operands = (
        source_feats,
        weight_neigh,
        hub_feats,
        send_rows[0].T,
        hub_source,
        hub_target,
        edge_target,
        edge_slot,
        target_feats,
        weight_self,
        bias_vector.reshape(1, width),
    )
    dma = pltpu.SemaphoreType.DMA
    vmem = pl.BlockSpec(memory_space=pltpu.VMEM)
    return pl.pallas_call(
        functools.partial(kernel, ny, nr),
        out_shape=(
            jax.ShapeDtypeStruct((targets, width), BF),
            jax.ShapeDtypeStruct((mine, width), BF),
        ),
        in_specs=[pl.BlockSpec(memory_space=pltpu.HBM)] * 11,
        out_specs=(vmem, vmem),
        scratch_shapes=[pltpu.VMEM(a.shape, a.dtype) for a in operands]
        + [
            pltpu.VMEM((NZ * NX, cap), F32),
            pltpu.VMEM((NZ, rows, width), BF),
            pltpu.VMEM((NZ, NZ, NX * cap), BF),
            pltpu.VMEM((NZ, NX * cap, width), BF),
            pltpu.VMEM((slots, width), BF),
            pltpu.VMEM((hubs, width + LANES), F32),
            pltpu.VMEM((group, mine, width + LANES), F32),
            pltpu.VMEM((targets, edges), F8),
            pltpu.VMEM((slots // LANES, targets, 2 * LANES), BF),
            pltpu.VMEM((targets, 2 * LANES), F32),
            pltpu.VMEM((targets, LANES), F32),
            pltpu.VMEM((targets, width), F32),
            pltpu.VMEM((targets, width), F32),
            pltpu.VMEM((2, half - RING, NX * cap, width), BF),
            dma((2, RING, CHUNKS)),
            dma((2, RING, CHUNKS)),
            dma((2, RING)),
            dma((2, RING)),
            dma((NX - 1, NZ)),
            dma((NX - 1, NZ)),
            dma((group - 1,)),
            dma((group - 1,)),
            dma((group - 1,)),
            dma((group - 1,)),
            dma((2, half - RING)),
            dma((2, half - RING)),
            dma((2, half - RING, NX)),
            dma((2, half - RING, NX)),
            dma((len(operands),)),
        ],
        compiler_params=pltpu.CompilerParams(
            collective_id=0, has_side_effects=True, vmem_limit_bytes=67043328
        ),
    )(*operands)


def solution(mesh):
    rows = P(("blk", "hub", "rep"), None)
    in_specs = (
        rows, rows, rows, P(), P(), P(),
        P(("blk", "hub", "rep"), None, None),
        rows, rows, rows, rows,
    )
    return jax.shard_map(
        on_device, mesh=mesh, in_specs=in_specs, out_specs=(rows, rows), check_vma=False
    )
```
